256 devices in a mesh: state: 256 (over y, z, x, core).
Axes of the slice: x: 4, y: 4, z: 8, core: 2. Of those that a mesh axis runs over, the one named last changes fastest.
Arguments:
- transitions: float32 [4096, 16, 4096], P('state'), may hold values from 0 to 1, as said below
- costs: float32 [4096, 16, 128], P('state'), may hold values from 0 to 4
- valid_counts: int32 [4096], P('state'), may hold values from 1 to 16
- start_values: float32 [4096, 128], P('state'), may hold values from -12 to 12
- ref_state: int32 [1], replicated, may hold values from 0 to 4095
Outputs:
- relative_values: float32 [4096, 128], P('state')
- lower_bounds: float32 [4, 128], replicated
- upper_bounds: float32 [4, 128], replicated
The draws below stay inside these ranges and needn't reach their ends.
Inputs may be any that keep to these rules, and one draw needn't show every extreme that they name: Every entry is nonnegative and each row transitions[s, a, :] sums to one up to float32 rounding. Actions 0 to valid_counts[s] - 1 are allowed in state s.
All inputs are finite; a program needn't handle non-finite values.
Results may differ from the reference program's by a relative error of at most 0.00017.
Values sent between devices are 32-bit elements; how exact they have to be, the bound alone decides.
No kernel may reach another device: no remote copies, remote signals or barrier semaphores. Data moves between devices by JAX's collectives and lax.ppermute only.
A program may use at most 64 MiB of HBM per device.

```python
import jax
import jax.numpy as jnp
from jax import lax

STATES = 4096
ACTIONS = 16
SCENARIOS = 128
ITERS = 4


def draw_transitions(key, part):
    sigma = 2.0
    raw = jnp.exp(sigma * jax.random.normal(key, (STATES, ACTIONS, STATES), jnp.float32))
    return raw / jnp.sum(raw, axis=2, keepdims=True)


def place_ends(values, stream_key, low, top_value):
    extent = values.shape
    index_at = [jax.random.randint(jax.random.fold_in(stream_key, axis), (), 0, extent[axis]) for axis in range(len(extent))]
    values = values.at[tuple(index_at)].set(low)
    longest = extent.index(max(extent))
    index_at[longest] = (index_at[longest] + 1) % extent[longest]
    return values.at[tuple(index_at)].set(top_value)


def level_of(stream_key, dims, cuts, low, largest):
    def one(position, blocks):
        steps = jax.random.uniform(jax.random.fold_in(jax.random.fold_in(stream_key, 6), position), (blocks,), jnp.float32, low / len(cuts), largest / len(cuts))
        return jnp.repeat(jnp.exp(steps), dims[position] // blocks).reshape((-1,) + (1,) * (len(dims) - position - 1))

    factor_of = one(*cuts[0])
    for cut in cuts[1:]:
        factor_of = factor_of * one(*cut)
    return factor_of


def normal_values(stream_key, dims, deviation, bound, shards=(), held_as=jnp.bfloat16):
    loudness = level_of(stream_key, dims, shards, -0.22, 0.18) if shards else 1.0
    values = jax.random.normal(stream_key, dims, jnp.float32) * deviation * loudness
    return jnp.minimum(jnp.maximum(values, -bound), bound).astype(held_as)


def setup_inputs(seed: int = 0) -> dict:
    streams_of = jax.random.split(jax.random.key(seed), 6)
    return {
        "transitions": draw_transitions(jax.random.fold_in(streams_of[5], 71), 0),
        "costs": jnp.clip(4.0 * jax.random.uniform(streams_of[1], (STATES, ACTIONS, SCENARIOS), jnp.float32) ** level_of(streams_of[1], (STATES, ACTIONS, SCENARIOS), ((0, 256),), -0.2, 0.2), 0.0, 4.0),
        "valid_counts": place_ends(jax.random.randint(streams_of[2], (STATES,), 1, ACTIONS + 1), jax.random.fold_in(streams_of[2], 1), 1, ACTIONS).astype(jnp.int32),
        "start_values": normal_values(streams_of[3], (STATES, SCENARIOS), 2.0, 12.0, ((0, 256),), jnp.float32),
        "ref_state": jax.random.randint(streams_of[4], (1,), 0, STATES).astype(jnp.int32),
    }


big_value = 1e30


def reference(transitions, costs, valid_counts, start_values, ref_state):
    flat_rows = transitions.reshape(STATES * ACTIONS, STATES)
    allowed = jnp.arange(ACTIONS, dtype=jnp.int32)[None, :] < valid_counts[:, None]
    relative = start_values
    lower_list = []
    upper_list = []
    for iteration in range(ITERS):
        expected = jnp.dot(flat_rows, relative, precision=lax.Precision.HIGHEST, preferred_element_type=jnp.float32)
        q_values = costs + expected.reshape(STATES, ACTIONS, SCENARIOS)
        q_values = jnp.where(allowed[:, :, None], q_values, jnp.float32(big_value))
        best_value = jnp.min(q_values, axis=1)
        increase = best_value - relative
        lower_list.append(jnp.min(increase, axis=0))
        upper_list.append(jnp.max(increase, axis=0))
        ref_row = lax.dynamic_slice_in_dim(best_value, ref_state[0].astype(jnp.int32), 1, 0)
        relative = best_value - ref_row
    return relative, jnp.stack(lower_list), jnp.stack(upper_list)
```

```python
import functools

import jax
import jax.numpy as jnp
from jax import lax
from jax.experimental import pallas as pl
from jax.experimental.pallas import tpu as pltpu
from jax.sharding import Mesh
from jax.sharding import PartitionSpec as P

ITERS = 4
YS, ZS, XS, CS = 4, 8, 4, 2
ROWS = 16
AXES = ("y", "z", "x", "c")
big_value = 1e30


def split_kernel(p_ref, out_ref):
    p = p_ref[...]
    high = p.astype(jnp.bfloat16)
    out_ref[0] = high
    out_ref[1] = (p - high.astype(jnp.float32)).astype(jnp.bfloat16)


def split_rows(flat_rows):
    m, k = flat_rows.shape
    step = m // 8
    return pl.pallas_call(
        split_kernel,
        grid=(8,),
        in_specs=[pl.BlockSpec((step, k), lambda i: (i, 0))],
        out_specs=pl.BlockSpec((2, step, k), lambda i: (0, i, 0)),
        out_shape=jax.ShapeDtypeStruct((2, m, k), jnp.bfloat16),
        compiler_params=pltpu.CompilerParams(vmem_limit_bytes=8 << 20),
        name="split_rows",
    )(flat_rows)


def bellman_kernel(core_ref, own_ref, other_ref, p_ref, costs_ref, best_ref, spread_ref, field):
    core = core_ref[0]

    def place(i, carry):
        y = i // ZS
        z = i % ZS
        for x in range(XS):
            base = (i * XS + x) * (CS * ROWS)
            for src, c in ((own_ref, core), (other_ref, 1 - core)):
                v = src[y * XS + x, pl.ds(pl.multiple_of(z * ROWS, ROWS), ROWS), :]
                high = v.astype(jnp.bfloat16)
                low = (v - high.astype(jnp.float32)).astype(jnp.bfloat16)
                at = pl.ds(pl.multiple_of(base + c * ROWS, ROWS), ROWS)
                field[at, 0:128] = high
                field[at, 128:256] = low
        return carry

    lax.fori_loop(0, YS * ZS, place, 0)
    top = jnp.dot(p_ref[0], field[...], preferred_element_type=jnp.float32)
    bottom = jnp.dot(p_ref[1], field[:, 0:128], preferred_element_type=jnp.float32)
    expected = top[:, 0:128] + (top[:, 128:256] + bottom)
    q = costs_ref[...] + expected
    best = jnp.min(q.reshape(ROWS, q.shape[0] // ROWS, 128), axis=1)
    best_ref[...] = best
    for i in range(ZS):
        spread_ref[i] = best


def bellman(core, own, other, parts, costs):
    return pl.pallas_call(
        bellman_kernel,
        in_specs=[pl.BlockSpec(memory_space=pltpu.SMEM)] + [pl.BlockSpec(memory_space=pltpu.VMEM)] * 4,
        out_specs=[pl.BlockSpec(memory_space=pltpu.VMEM)] * 2,
        out_shape=[
            jax.ShapeDtypeStruct((ROWS, 128), jnp.float32),
            jax.ShapeDtypeStruct((ZS, ROWS, 128), jnp.float32),
        ],
        scratch_shapes=[pltpu.VMEM((4096, 256), jnp.bfloat16)],
        compiler_params=pltpu.CompilerParams(vmem_limit_bytes=24 << 20),
        name="bellman",
    )(core, own, other, parts, costs)


def gather(spread):
    block = lax.all_to_all(spread, "z", 0, 0, tiled=True).reshape(1, ZS * ROWS, 128)
    plane = jnp.broadcast_to(block, (YS * XS, ZS * ROWS, 128))
    own = lax.all_to_all(plane, ("y", "x"), 0, 0, tiled=True)
    other = lax.ppermute(own, "c", [(0, 1), (1, 0)])
    return own, other


def local(transitions, costs, valid_counts, start_values, ref_state):
    local_states = transitions.shape[0]
    actions = transitions.shape[1]
    flat_rows = transitions.reshape(local_states * actions, transitions.shape[2])
    allowed = jnp.arange(actions, dtype=jnp.int32)[None, :] < valid_counts[:, None]
    costs = jnp.where(allowed[:, :, None], costs, jnp.float32(big_value))
    costs = costs.reshape(local_states * actions, -1)
    parts = split_rows(flat_rows)
    my_index = lax.axis_index(AXES)
    core = lax.axis_index("c").reshape(1)
    first_state = my_index * local_states
    owner_index = ref_state[0] // local_states
    offset = jnp.clip(ref_state[0] - first_state, 0, local_states - 1)
    is_owner = owner_index == my_index
    value = start_values
    spread = jnp.broadcast_to(value[None], (ZS,) + value.shape)
    rows = []
    for _ in range(ITERS):
        own, other = gather(spread)
        best, spread = bellman(core, own, other, parts, costs)
        increase = best - value
        rows.append((jnp.max(increase, axis=0), jnp.max(-increase, axis=0)))
        value = best
    local_row = lax.dynamic_slice_in_dim(value, offset, 1, 0)
    ref_row = jnp.where(is_owner, local_row, jnp.float32(-big_value))
    ends = jnp.concatenate([jnp.stack([u for u, _ in rows]), jnp.stack([l for _, l in rows]), ref_row], axis=0)
    ends = jnp.pad(ends, ((0, 16 - ends.shape[0]), (0, 0)))
    ends = jnp.max(lax.all_to_all(jnp.broadcast_to(ends[None], (ZS,) + ends.shape), "z", 0, 0, tiled=True), axis=0)
    ends = jnp.max(lax.all_to_all(jnp.broadcast_to(ends[None], (YS * XS,) + ends.shape), ("y", "x"), 0, 0, tiled=True), axis=0)
    ends = jnp.maximum(ends, lax.ppermute(ends, "c", [(0, 1), (1, 0)]))
    return value - ends[2 * ITERS], -ends[ITERS : 2 * ITERS], ends[:ITERS]


def solution(mesh):
    split = Mesh(mesh.devices.reshape(YS, ZS, XS, CS), AXES)
    return jax.shard_map(
        local,
        mesh=split,
        in_specs=(P(AXES, None, None), P(AXES, None, None), P(AXES), P(AXES, None), P()),
        out_specs=(P(AXES, None), P(), P()),
        check_vma=False,
    )
```

```python
import functools

import jax
import jax.numpy as jnp
from jax import lax
from jax.experimental import pallas as pl
from jax.experimental.pallas import tpu as pltpu
from jax.sharding import Mesh
from jax.sharding import PartitionSpec as P

ITERS = 4
YS, ZS, XS, CS = 4, 8, 4, 2
ROWS = 16
HALF = 64
LANES = 128
AXES = ("y", "z", "x", "c")
SWAP = [(0, 1), (1, 0)]
big_value = 1e30

VMEM = pl.BlockSpec(memory_space=pltpu.VMEM)
SMEM = pl.BlockSpec(memory_space=pltpu.SMEM)
HBM = pl.BlockSpec(memory_space=pltpu.HBM)
TILE = jax.ShapeDtypeStruct((ROWS, LANES), jnp.float32)
SPREAD = jax.ShapeDtypeStruct((ZS, ROWS, LANES), jnp.float32)


def half_of(shape):
    return lax.broadcasted_iota(jnp.int32, shape, len(shape) - 1) // HALF


def merge(core, mine, theirs):
    return jnp.where(half_of(mine.shape) == core, mine, pltpu.roll(theirs, HALF, mine.ndim - 1))


def call(body, name, ins, outs, scratch=(), mib=16):
    return pl.pallas_call(
        body,
        in_specs=ins,
        out_specs=[VMEM] * len(outs) if isinstance(outs, list) else VMEM,
        out_shape=outs,
        scratch_shapes=scratch,
        compiler_params=pltpu.CompilerParams(vmem_limit_bytes=mib << 20),
        name=name,
    )


def begin_kernel(
    ref_ref, my_counts_ref, their_counts_ref, my_costs_ref, their_costs_ref, my_start_ref, their_start_ref,
    value_ref, spread_ref, costs_out, ref_out,
):
    core = lax.axis_index("c")
    value = merge(core, my_start_ref[...], their_start_ref[...])
    value_ref[...] = value
    for i in range(ZS):
        spread_ref[i] = value
    actions = my_costs_ref.shape[1]
    action = lax.broadcasted_iota(jnp.int32, (actions, LANES), 0)
    for s in range(ROWS):
        mine = jnp.where(action < my_counts_ref[s], my_costs_ref[s], big_value)
        theirs = jnp.where(action < their_counts_ref[s], their_costs_ref[s], big_value)
        costs_out[s * actions : (s + 1) * actions, :] = merge(core, mine, theirs)
    ref_out[...] = jnp.full((ROWS, LANES), ref_ref[0], jnp.int32)


def place(blocks_ref, field):
    left = half_of((ROWS, LANES)) == 0
    for i in range(YS * ZS * XS):
        y, z, x = i // (ZS * XS), i // XS % ZS, i % XS
        v = blocks_ref[y * XS + x, z * ROWS : (z + 1) * ROWS, :]
        w = pltpu.roll(v, HALF, 1)
        for c, u in enumerate((jnp.where(left, v, w), jnp.where(left, w, v))):
            high = u.astype(jnp.bfloat16).astype(jnp.float32)
            at = (i * CS + c) * ROWS
            field[at : at + ROWS, :] = jnp.where(left, high, u - high).astype(jnp.bfloat16)


def product(high, low, field):
    total = jnp.dot(high, field, preferred_element_type=jnp.float32)
    return total + jnp.dot(low, field, preferred_element_type=jnp.float32)


def finish(t, mine, theirs, costs, value_ref, ends_ref, ref_ref, best_ref, spread_ref, ends_out):
    core = lax.axis_index("c")
    mine = mine + pltpu.roll(mine, HALF, 1)
    theirs = theirs + pltpu.roll(theirs, HALF, 1)
    q = costs + jnp.where(half_of(mine.shape) == core, mine, theirs)
    best = jnp.min(q.reshape(ROWS, q.shape[0] // ROWS, LANES), axis=1)
    increase = best - value_ref[...]
    row = lax.broadcasted_iota(jnp.int32, (ROWS, LANES), 0)
    old = jnp.full((ROWS, LANES), -big_value, jnp.float32) if ends_ref is None else ends_ref[...]
    ends = jnp.where(row == t, jnp.max(increase, axis=0, keepdims=True), old)
    ends = jnp.where(row == ITERS + t, jnp.max(-increase, axis=0, keepdims=True), ends)
    best_ref[...] = best
    if t < ITERS - 1:
        ends_out[...] = ends
        for i in range(ZS):
            spread_ref[i] = best
        return
    chip = (lax.axis_index("y") * ZS + lax.axis_index("z")) * XS + lax.axis_index("x")
    owner = (row + ROWS * (CS * chip + half_of((ROWS, LANES)))) == ref_ref[...]
    ref_row = jnp.max(jnp.where(owner, best, -big_value), axis=0, keepdims=True)
    ends = jnp.where(row == 2 * ITERS, ref_row, ends)
    for i in range(ZS):
        spread_ref[i] = ends


def first_kernel(
    blocks_ref, mine_hbm, theirs_ref, costs_ref, value_ref,
    best_ref, spread_ref, ends_out, mine_out, theirs_out,
    field, mine_rows, sems,
):
    chunk = mine_rows.shape[1]
    copies = []
    for j in range(mine_rows.shape[0]):
        copy = pltpu.make_async_copy(mine_hbm.at[pl.ds(j * chunk, chunk)], mine_rows.at[j], sems.at[j])
        copy.start()
        copies.append(copy)
    place(blocks_ref, field)

    def part(p, out, j):
        at = slice(j * chunk, (j + 1) * chunk)
        high = p.astype(jnp.bfloat16)
        out[0, at, :] = high
        out[1, at, :] = (p - high.astype(jnp.float32)).astype(jnp.bfloat16)
        return product(out[0, at, :], out[1, at, :], field[...])

    theirs = jnp.concatenate(
        [part(theirs_ref[j * chunk : (j + 1) * chunk, :], theirs_out, j) for j in range(len(copies))], axis=0
    )
    mine = []
    for j, copy in enumerate(copies):
        copy.wait()
        mine.append(part(mine_rows[j], mine_out, j))
    mine = jnp.concatenate(mine, axis=0)
    finish(0, mine, theirs, costs_ref[...], value_ref, None, None, best_ref, spread_ref, ends_out)


def bellman_kernel(t, blocks_ref, mine_ref, theirs_ref, costs_ref, value_ref, ends_ref, *refs):
    ref_ref = refs[0] if t == ITERS - 1 else None
    *outs, field = refs[1:] if t == ITERS - 1 else refs
    place(blocks_ref, field)
    mine = product(mine_ref[0], mine_ref[1], field[...])
    theirs = product(theirs_ref[0], theirs_ref[1], field[...])
    ends_out = None if t == ITERS - 1 else outs[2]
    finish(t, mine, theirs, costs_ref[...], value_ref, ends_ref, ref_ref, outs[0], outs[1], ends_out)


def reduce_kernel(parts_ref, out_ref):
    ends = jnp.max(parts_ref[...], axis=0)
    for i in range(YS * XS):
        out_ref[i] = ends


def packet_kernel(parts_ref, value_ref, out_ref):
    ends = jnp.max(parts_ref[...], axis=0)
    ends = jnp.maximum(ends, pltpu.roll(ends, HALF, 1))
    out_ref[0:ROWS, :] = value_ref[...] - ends[2 * ITERS : 2 * ITERS + 1, :]
    out_ref[ROWS : ROWS + 2 * ITERS, :] = ends[0 : 2 * ITERS, :]


def unpack_kernel(mine_ref, theirs_ref, relative_ref, lower_ref, upper_ref):
    core = lax.axis_index("c")
    relative_ref[...] = merge(core, mine_ref[0:ROWS, :], theirs_ref[0:ROWS, :])
    bounds = jnp.where(
        half_of((2 * ITERS, LANES)) == core,
        mine_ref[ROWS : ROWS + 2 * ITERS, :],
        theirs_ref[ROWS : ROWS + 2 * ITERS, :],
    )
    upper_ref[...] = bounds[:ITERS]
    lower_ref[...] = -bounds[ITERS:]


def gather(spread):
    block = lax.all_to_all(spread, "z", 0, 0, tiled=True).reshape(1, ZS * ROWS, LANES)
    plane = jnp.broadcast_to(block, (YS * XS, ZS * ROWS, LANES))
    return lax.all_to_all(plane, ("y", "x"), 0, 0, tiled=True)


def swap(value):
    return lax.ppermute(value, "c", SWAP)


def local(transitions, costs, valid_counts, start_values, ref_state):
    states, actions, total_states = transitions.shape
    m = states * actions
    flat_rows = transitions.reshape(m, total_states)
    value, spread, costs, ref_rows = call(
        begin_kernel,
        "begin",
        [SMEM] * 3 + [VMEM] * 4,
        [TILE, SPREAD, pltpu.VMEM((m, LANES), jnp.float32), jax.ShapeDtypeStruct((ROWS, LANES), jnp.int32)],
    )(ref_state, valid_counts, swap(valid_counts), costs, swap(costs), start_values, swap(start_values))
    flat_rows, value, spread, costs = lax.optimization_barrier((flat_rows, value, spread, costs))
    their_rows = swap(flat_rows)
    my_rows = pltpu.with_memory_space_constraint(flat_rows, pltpu.HBM)
    parts = pltpu.VMEM((2, m, total_states), jnp.bfloat16)
    field = pltpu.VMEM((total_states, LANES), jnp.bfloat16)
    count = 2
    value, spread, ends, mine, theirs = call(
        first_kernel,
        "bellman_0",
        [VMEM, HBM, VMEM, VMEM, VMEM],
        [TILE, SPREAD, TILE, parts, parts],
        [field, pltpu.VMEM((count, m // count, total_states), jnp.float32), pltpu.SemaphoreType.DMA((count,))],
        32,
    )(gather(spread), my_rows, their_rows, costs, value)
    mine = pltpu.with_memory_space_constraint(mine, pltpu.VMEM)
    theirs = pltpu.with_memory_space_constraint(theirs, pltpu.VMEM)
    for t in range(1, ITERS):
        last = t == ITERS - 1
        outs = call(
            functools.partial(bellman_kernel, t),
            f"bellman_{t}",
            [VMEM] * (6 + last),
            [TILE, SPREAD] + [TILE] * (not last),
            [field],
        )(gather(spread), mine, theirs, costs, value, ends, *([ref_rows] * last))
        value, spread = outs[:2]
        ends = None if last else outs[2]
    rows = lax.all_to_all(spread, "z", 0, 0, tiled=True)
    plane = call(reduce_kernel, "reduce", [VMEM], jax.ShapeDtypeStruct((YS * XS, ROWS, LANES), jnp.float32))(rows)
    rows = lax.all_to_all(plane, ("y", "x"), 0, 0, tiled=True)
    packet = call(packet_kernel, "packet", [VMEM] * 2, jax.ShapeDtypeStruct((ROWS + 2 * ITERS, LANES), jnp.float32))(rows, value)
    bound = jax.ShapeDtypeStruct((ITERS, LANES), jnp.float32)
    return tuple(call(unpack_kernel, "unpack", [VMEM] * 2, [TILE, bound, bound])(packet, swap(packet)))


def solution(mesh):
    split = Mesh(mesh.devices.reshape(YS, ZS, XS, CS), AXES)
    return jax.shard_map(
        local,
        mesh=split,
        in_specs=(P(AXES, None, None), P(AXES, None, None), P(AXES), P(AXES, None), P()),
        out_specs=(P(AXES, None), P(), P()),
        check_vma=False,
    )
```

```python
import functools

import jax
import jax.numpy as jnp
from jax import lax
from jax.experimental import pallas as pl
from jax.experimental.pallas import tpu as pltpu
from jax.sharding import Mesh
from jax.sharding import PartitionSpec as P

ITERS = 4
YS, ZS, XS, CS = 4, 8, 4, 2
ROWS = 16
HALF = 64
LANES = 128
AXES = ("y", "z", "x", "c")
SWAP = [(0, 1), (1, 0)]
big_value = 1e30

VMEM = pl.BlockSpec(memory_space=pltpu.VMEM)
SMEM = pl.BlockSpec(memory_space=pltpu.SMEM)
HBM = pl.BlockSpec(memory_space=pltpu.HBM)
TILE = jax.ShapeDtypeStruct((ROWS, LANES), jnp.float32)
SPREAD = jax.ShapeDtypeStruct((ZS, ROWS, LANES), jnp.float32)


def half_of(shape):
    return lax.broadcasted_iota(jnp.int32, shape, len(shape) - 1) // HALF


def merge(core, mine, theirs):
    return jnp.where(half_of(mine.shape) == core, mine, pltpu.roll(theirs, HALF, mine.ndim - 1))


def call(body, name, ins, outs, scratch=(), mib=16):
    return pl.pallas_call(
        body,
        in_specs=ins,
        out_specs=[VMEM] * len(outs) if isinstance(outs, list) else VMEM,
        out_shape=outs,
        scratch_shapes=scratch,
        compiler_params=pltpu.CompilerParams(vmem_limit_bytes=mib << 20),
        name=name,
    )


def begin_kernel(
    my_counts_hbm, my_costs_hbm, my_start_hbm, ref_ref, their_counts_ref, their_costs_ref, their_start_ref,
    value_ref, spread_ref, costs_out, ref_out,
    my_counts_ref, my_costs_ref, my_start_ref, sems,
):
    pairs = (
        (my_start_hbm, my_start_ref),
        (my_costs_hbm, my_costs_ref),
        (my_counts_hbm, my_counts_ref),
    )
    copies = [pltpu.make_async_copy(src, dst, sems.at[j]) for j, (src, dst) in enumerate(pairs)]
    for copy in copies:
        copy.start()
    core = lax.axis_index("c")
    copies[0].wait()
    value = merge(core, my_start_ref[...], their_start_ref[...])
    value_ref[...] = value
    for i in range(ZS):
        spread_ref[i] = value
    for copy in copies[1:]:
        copy.wait()
    actions = my_costs_ref.shape[1]
    action = lax.broadcasted_iota(jnp.int32, (actions, LANES), 0)
    for s in range(ROWS):
        mine = jnp.where(action < my_counts_ref[s], my_costs_ref[s], big_value)
        theirs = jnp.where(action < their_counts_ref[s], their_costs_ref[s], big_value)
        costs_out[s * actions : (s + 1) * actions, :] = merge(core, mine, theirs)
    ref_out[...] = jnp.full((ROWS, LANES), ref_ref[0], jnp.int32)


def place(blocks_ref, field, old_ref=None):
    left = half_of((ROWS, LANES)) == 0
    high_end = low_end = None
    for i in range(YS * ZS * XS):
        y, z, x = i // (ZS * XS), i // XS % ZS, i % XS
        block = (y * XS + x, slice(z * ROWS, (z + 1) * ROWS))
        v = blocks_ref[block]
        if old_ref is not None:
            increase = v - old_ref[block]
            high_end = increase if i == 0 else jnp.maximum(high_end, increase)
            low_end = increase if i == 0 else jnp.minimum(low_end, increase)
        w = pltpu.roll(v, HALF, 1)
        for c, u in enumerate((jnp.where(left, v, w), jnp.where(left, w, v))):
            high = u.astype(jnp.bfloat16).astype(jnp.float32)
            at = (i * CS + c) * ROWS
            field[at : at + ROWS, :] = jnp.where(left, high, u - high).astype(jnp.bfloat16)
    if old_ref is None:
        return None
    return both_halves(jnp.max(high_end, axis=0, keepdims=True)), both_halves(jnp.max(-low_end, axis=0, keepdims=True))


def both_halves(row):
    return jnp.maximum(row, pltpu.roll(row, HALF, 1))


def product(high, low, field):
    total = jnp.dot(high, field, preferred_element_type=jnp.float32)
    return total + jnp.dot(low, field, preferred_element_type=jnp.float32)


def improve(mine, theirs, costs):
    mine = mine + pltpu.roll(mine, HALF, 1)
    theirs = theirs + pltpu.roll(theirs, HALF, 1)
    q = costs + jnp.where(half_of(mine.shape) == lax.axis_index("c"), mine, theirs)
    return jnp.min(q.reshape(ROWS, q.shape[0] // ROWS, LANES), axis=1)


def first_kernel(
    blocks_ref, mine_hbm, theirs_ref, costs_ref,
    spread_ref, mine_out, theirs_out,
    field, mine_rows, sems,
):
    chunk = mine_rows.shape[1]
    copies = []
    for j in range(mine_rows.shape[0]):
        copy = pltpu.make_async_copy(mine_hbm.at[pl.ds(j * chunk, chunk)], mine_rows.at[j], sems.at[j])
        copy.start()
        copies.append(copy)
    place(blocks_ref, field)

    def part(p, out, j):
        at = slice(j * chunk, (j + 1) * chunk)
        high = p.astype(jnp.bfloat16)
        out[0, at, :] = high
        out[1, at, :] = (p - high.astype(jnp.float32)).astype(jnp.bfloat16)
        return product(out[0, at, :], out[1, at, :], field[...])

    theirs = jnp.concatenate(
        [part(theirs_ref[j * chunk : (j + 1) * chunk, :], theirs_out, j) for j in range(len(copies))], axis=0
    )
    mine = []
    for j, copy in enumerate(copies):
        copy.wait()
        mine.append(part(mine_rows[j], mine_out, j))
    mine = jnp.concatenate(mine, axis=0)
    best = improve(mine, theirs, costs_ref[...])
    for i in range(ZS):
        spread_ref[i] = best


def bellman_kernel(t, blocks_ref, old_ref, mine_ref, theirs_ref, costs_ref, ends_ref, *refs):
    last = t == ITERS - 1
    spread_ref, ends_out, field = refs[-3:]
    up, down = place(blocks_ref, field, old_ref)
    mine = product(mine_ref[0], mine_ref[1], field[...])
    theirs = product(theirs_ref[0], theirs_ref[1], field[...])
    best = improve(mine, theirs, costs_ref[...])
    row = lax.broadcasted_iota(jnp.int32, (2 * ITERS, LANES), 0)
    ends = jnp.zeros((2 * ITERS, LANES), jnp.float32) if t == 1 else ends_ref[...]
    ends = jnp.where(row == t - 1, up, ends)
    ends_out[...] = jnp.where(row == ITERS + t - 1, down, ends)
    if not last:
        for i in range(ZS):
            spread_ref[i] = best
        return
    ref_ref, value_ref, best_ref = refs[:3]
    increase = best - value_ref[0]
    up = both_halves(jnp.max(increase, axis=0, keepdims=True))
    down = both_halves(jnp.max(-increase, axis=0, keepdims=True))
    chip = (lax.axis_index("y") * ZS + lax.axis_index("z")) * XS + lax.axis_index("x")
    state = lax.broadcasted_iota(jnp.int32, (ROWS, LANES), 0) + ROWS * (CS * chip + half_of((ROWS, LANES)))
    ref_row = both_halves(jnp.max(jnp.where(state == ref_ref[...], best, -big_value), axis=0, keepdims=True))
    best_ref[...] = best
    pair = jnp.concatenate([jnp.where(half_of((1, LANES)) == 0, up, down), ref_row], axis=0)
    spread_ref[...] = jnp.broadcast_to(pair[None], spread_ref.shape)


def packet_kernel(parts_ref, value_ref, ends_ref, out_ref):
    pair = jnp.max(parts_ref[...], axis=0)
    out_ref[0:ROWS, :] = value_ref[...] - pair[1:2, :]
    turned = pltpu.roll(pair, HALF, 1)
    left = half_of((1, LANES)) == 0
    row = lax.broadcasted_iota(jnp.int32, (2 * ITERS, LANES), 0)
    ends = jnp.where(row == ITERS - 1, jnp.where(left, pair[0:1, :], turned[0:1, :]), ends_ref[...])
    ends = jnp.where(row == 2 * ITERS - 1, jnp.where(left, turned[0:1, :], pair[0:1, :]), ends)
    out_ref[ROWS : ROWS + 2 * ITERS, :] = ends


def unpack_kernel(mine_ref, theirs_ref, relative_ref, lower_ref, upper_ref):
    core = lax.axis_index("c")
    relative_ref[...] = merge(core, mine_ref[0:ROWS, :], theirs_ref[0:ROWS, :])
    bounds = jnp.where(
        half_of((2 * ITERS, LANES)) == core,
        mine_ref[ROWS : ROWS + 2 * ITERS, :],
        theirs_ref[ROWS : ROWS + 2 * ITERS, :],
    )
    upper_ref[...] = bounds[:ITERS]
    lower_ref[...] = -bounds[ITERS:]


def gather(spread):
    block = lax.all_to_all(spread, "z", 0, 0, tiled=True).reshape(1, ZS * ROWS, LANES)
    plane = jnp.broadcast_to(block, (YS * XS, ZS * ROWS, LANES))
    return lax.all_to_all(plane, ("y", "x"), 0, 0, tiled=True)


def swap(value):
    return lax.ppermute(value, "c", SWAP)


def local(transitions, costs, valid_counts, start_values, ref_state):
    states, actions, total_states = transitions.shape
    m = states * actions
    flat_rows = transitions.reshape(m, total_states)
    value, spread, costs, ref_rows = call(
        begin_kernel,
        "begin",
        [HBM] * 3 + [SMEM] * 2 + [VMEM] * 2,
        [TILE, SPREAD, pltpu.VMEM((m, LANES), jnp.float32), jax.ShapeDtypeStruct((ROWS, LANES), jnp.int32)],
        [
            pltpu.SMEM(valid_counts.shape, jnp.int32),
            pltpu.VMEM(costs.shape, jnp.float32),
            pltpu.VMEM(start_values.shape, jnp.float32),
            pltpu.SemaphoreType.DMA((3,)),
        ],
    )(
        *(pltpu.with_memory_space_constraint(v, pltpu.HBM) for v in (valid_counts, costs, start_values)),
        ref_state,
        *(swap(v) for v in (valid_counts, costs, start_values)),
    )
    flat_rows, value, spread, costs = lax.optimization_barrier((flat_rows, value, spread, costs))
    their_rows = swap(flat_rows)
    my_rows = pltpu.with_memory_space_constraint(flat_rows, pltpu.HBM)
    parts = pltpu.VMEM((2, m, total_states), jnp.bfloat16)
    field = pltpu.VMEM((total_states, LANES), jnp.bfloat16)
    count = 2
    old = gather(spread)
    spread, mine, theirs = call(
        first_kernel,
        "bellman_0",
        [VMEM, HBM, VMEM, VMEM],
        [SPREAD, parts, parts],
        [field, pltpu.VMEM((count, m // count, total_states), jnp.float32), pltpu.SemaphoreType.DMA((count,))],
        32,
    )(old, my_rows, their_rows, costs)
    mine = pltpu.with_memory_space_constraint(mine, pltpu.VMEM)
    theirs = pltpu.with_memory_space_constraint(theirs, pltpu.VMEM)
    ends_shape = jax.ShapeDtypeStruct((2 * ITERS, LANES), jnp.float32)
    ends = value
    for t in range(1, ITERS):
        last = t == ITERS - 1
        blocks = gather(spread)
        pairs = jax.ShapeDtypeStruct((YS * ZS * XS, 2, LANES), jnp.float32)
        outs = call(
            functools.partial(bellman_kernel, t),
            f"bellman_{t}",
            [VMEM] * (8 if last else 6),
            [TILE, pairs, ends_shape] if last else [SPREAD, ends_shape],
            [field],
        )(blocks, old, mine, theirs, costs, ends, *([ref_rows, spread] if last else []))
        spread, ends = outs[-2:]
        old = blocks
    rows = lax.all_to_all(spread, ("y", "z", "x"), 0, 0, tiled=True)
    packet = call(packet_kernel, "packet", [VMEM] * 3, jax.ShapeDtypeStruct((ROWS + 2 * ITERS, LANES), jnp.float32))(
        rows, outs[0], ends
    )
    bound = jax.ShapeDtypeStruct((ITERS, LANES), jnp.float32)
    return tuple(call(unpack_kernel, "unpack", [VMEM] * 2, [TILE, bound, bound])(packet, swap(packet)))


def solution(mesh):
    split = Mesh(mesh.devices.reshape(YS, ZS, XS, CS), AXES)
    return jax.shard_map(
        local,
        mesh=split,
        in_specs=(P(AXES, None, None), P(AXES, None, None), P(AXES), P(AXES, None), P()),
        out_specs=(P(AXES, None), P(), P()),
        check_vma=False,
    )
```

```python
import functools

import jax
import jax.numpy as jnp
from jax import lax
from jax.experimental import pallas as pl
from jax.experimental.pallas import tpu as pltpu
from jax.sharding import Mesh
from jax.sharding import PartitionSpec as P

ITERS = 4
YS, ZS, XS, CS = 4, 8, 4, 2
ROWS = 16
HALF = 64
LANES = 128
AXES = ("y", "z", "x", "c")
SWAP = [(0, 1), (1, 0)]
big_value = 1e30

VMEM = pl.BlockSpec(memory_space=pltpu.VMEM)
SMEM = pl.BlockSpec(memory_space=pltpu.SMEM)
HBM = pl.BlockSpec(memory_space=pltpu.HBM)
TILE = jax.ShapeDtypeStruct((ROWS, LANES), jnp.float32)
SPREAD = jax.ShapeDtypeStruct((ZS, ROWS, LANES), jnp.float32)


def half_of(shape):
    return lax.broadcasted_iota(jnp.int32, shape, len(shape) - 1) // HALF


def merge(core, mine, theirs):
    return jnp.where(half_of(mine.shape) == core, mine, pltpu.roll(theirs, HALF, mine.ndim - 1))


def call(body, name, ins, outs, scratch=(), mib=16):
    return pl.pallas_call(
        body,
        in_specs=ins,
        out_specs=[VMEM] * len(outs) if isinstance(outs, list) else VMEM,
        out_shape=outs,
        scratch_shapes=scratch,
        compiler_params=pltpu.CompilerParams(vmem_limit_bytes=mib << 20),
        name=name,
    )


def begin_kernel(ref_ref, my_start_hbm, their_start_ref, value_ref, spread_ref, ref_out, my_start_ref, sem):
    copy = pltpu.make_async_copy(my_start_hbm, my_start_ref, sem)
    copy.start()
    ref_out[...] = jnp.full((ROWS, LANES), ref_ref[0], jnp.int32)
    copy.wait()
    value = merge(lax.axis_index("c"), my_start_ref[...], their_start_ref[...])
    value_ref[...] = value
    for i in range(ZS):
        spread_ref[i] = value


def place(blocks_ref, field, old_ref=None):
    left = half_of((ROWS, LANES)) == 0
    high_end = low_end = None
    for i in range(YS * ZS * XS):
        y, z, x = i // (ZS * XS), i // XS % ZS, i % XS
        block = (y * XS + x, slice(z * ROWS, (z + 1) * ROWS))
        v = blocks_ref[block]
        if old_ref is not None:
            increase = v - old_ref[block]
            high_end = increase if i == 0 else jnp.maximum(high_end, increase)
            low_end = increase if i == 0 else jnp.minimum(low_end, increase)
        w = pltpu.roll(v, HALF, 1)
        for c, u in enumerate((jnp.where(left, v, w), jnp.where(left, w, v))):
            high = u.astype(jnp.bfloat16).astype(jnp.float32)
            at = (i * CS + c) * ROWS
            field[at : at + ROWS, :] = jnp.where(left, high, u - high).astype(jnp.bfloat16)
    if old_ref is None:
        return None
    return both_halves(jnp.max(high_end, axis=0, keepdims=True)), both_halves(jnp.max(-low_end, axis=0, keepdims=True))


def both_halves(row):
    return jnp.maximum(row, pltpu.roll(row, HALF, 1))


def product(high, low, field):
    total = jnp.dot(high, field, preferred_element_type=jnp.float32)
    return total + jnp.dot(low, field, preferred_element_type=jnp.float32)


def improve(mine, theirs, costs):
    mine = mine + pltpu.roll(mine, HALF, 1)
    theirs = theirs + pltpu.roll(theirs, HALF, 1)
    q = costs + jnp.where(half_of(mine.shape) == lax.axis_index("c"), mine, theirs)
    return jnp.min(q.reshape(ROWS, q.shape[0] // ROWS, LANES), axis=1)


def first_kernel(
    blocks_ref, mine_hbm, theirs_ref, my_counts_hbm, their_counts_ref, my_costs_hbm, their_costs_ref,
    spread_ref, mine_out, theirs_out, costs_out,
    field, mine_rows, my_counts_ref, my_costs_ref, sems, small_sems,
):
    small = [
        pltpu.make_async_copy(my_counts_hbm, my_counts_ref, small_sems.at[0]),
        pltpu.make_async_copy(my_costs_hbm, my_costs_ref, small_sems.at[1]),
    ]
    for copy in small:
        copy.start()
    wide = mine_rows.shape[2]
    copies = []
    for j in range(mine_rows.shape[0]):
        copy = pltpu.make_async_copy(mine_hbm.at[:, pl.ds(j * wide, wide)], mine_rows.at[j], sems.at[j])
        copy.start()
        copies.append(copy)
    place(blocks_ref, field)

    def part(p, out, j):
        at = slice(j * wide, (j + 1) * wide)
        high = p.astype(jnp.bfloat16)
        low = (p - high.astype(jnp.float32)).astype(jnp.bfloat16)
        out[0, :, at] = high
        out[1, :, at] = low
        return product(high, low, field[at, :])

    for copy in small:
        copy.wait()
    core = lax.axis_index("c")
    actions = my_costs_ref.shape[1]
    action = lax.broadcasted_iota(jnp.int32, (actions, LANES), 0)
    for s in range(ROWS):
        own = jnp.where(action < my_counts_ref[s], my_costs_ref[s], big_value)
        other = jnp.where(action < their_counts_ref[s], their_costs_ref[s], big_value)
        costs_out[s * actions : (s + 1) * actions, :] = merge(core, own, other)
    theirs = mine = 0.0
    for j in range(len(copies)):
        theirs = theirs + part(theirs_ref[:, j * wide : (j + 1) * wide], theirs_out, j)
    for j, copy in enumerate(copies):
        copy.wait()
        mine = mine + part(mine_rows[j], mine_out, j)
    best = improve(mine, theirs, costs_out[...])
    for i in range(ZS):
        spread_ref[i] = best


def bellman_kernel(t, blocks_ref, old_ref, mine_ref, theirs_ref, costs_ref, ends_ref, *refs):
    last = t == ITERS - 1
    spread_ref, ends_out, field = refs[-3:]
    up, down = place(blocks_ref, field, old_ref)
    mine = product(mine_ref[0], mine_ref[1], field[...])
    theirs = product(theirs_ref[0], theirs_ref[1], field[...])
    best = improve(mine, theirs, costs_ref[...])
    row = lax.broadcasted_iota(jnp.int32, (2 * ITERS, LANES), 0)
    ends = jnp.zeros((2 * ITERS, LANES), jnp.float32) if t == 1 else ends_ref[...]
    ends = jnp.where(row == t - 1, up, ends)
    ends_out[...] = jnp.where(row == ITERS + t - 1, down, ends)
    if not last:
        for i in range(ZS):
            spread_ref[i] = best
        return
    ref_ref, value_ref, best_ref = refs[:3]
    increase = best - value_ref[0]
    up = both_halves(jnp.max(increase, axis=0, keepdims=True))
    down = both_halves(jnp.max(-increase, axis=0, keepdims=True))
    chip = (lax.axis_index("y") * ZS + lax.axis_index("z")) * XS + lax.axis_index("x")
    state = lax.broadcasted_iota(jnp.int32, (ROWS, LANES), 0) + ROWS * (CS * chip + half_of((ROWS, LANES)))
    ref_row = both_halves(jnp.max(jnp.where(state == ref_ref[...], best, -big_value), axis=0, keepdims=True))
    best_ref[...] = best
    pair = jnp.concatenate([jnp.where(half_of((1, LANES)) == 0, up, down), ref_row], axis=0)
    spread_ref[...] = jnp.broadcast_to(pair[None], spread_ref.shape)


def packet_kernel(parts_ref, value_ref, ends_ref, out_ref):
    pair = jnp.max(parts_ref[...], axis=0)
    out_ref[0:ROWS, :] = value_ref[...] - pair[1:2, :]
    turned = pltpu.roll(pair, HALF, 1)
    left = half_of((1, LANES)) == 0
    row = lax.broadcasted_iota(jnp.int32, (2 * ITERS, LANES), 0)
    ends = jnp.where(row == ITERS - 1, jnp.where(left, pair[0:1, :], turned[0:1, :]), ends_ref[...])
    ends = jnp.where(row == 2 * ITERS - 1, jnp.where(left, turned[0:1, :], pair[0:1, :]), ends)
    out_ref[ROWS : ROWS + 2 * ITERS, :] = ends


def unpack_kernel(mine_ref, theirs_ref, relative_ref, lower_ref, upper_ref):
    core = lax.axis_index("c")
    relative_ref[...] = merge(core, mine_ref[0:ROWS, :], theirs_ref[0:ROWS, :])
    bounds = jnp.where(
        half_of((2 * ITERS, LANES)) == core,
        mine_ref[ROWS : ROWS + 2 * ITERS, :],
        theirs_ref[ROWS : ROWS + 2 * ITERS, :],
    )
    upper_ref[...] = bounds[:ITERS]
    lower_ref[...] = -bounds[ITERS:]


def gather(spread):
    block = lax.all_to_all(spread, "z", 0, 0, tiled=True).reshape(1, ZS * ROWS, LANES)
    plane = jnp.broadcast_to(block, (YS * XS, ZS * ROWS, LANES))
    return lax.all_to_all(plane, ("y", "x"), 0, 0, tiled=True)


def swap(value):
    return lax.ppermute(value, "c", SWAP)


def local(transitions, costs, valid_counts, start_values, ref_state):
    states, actions, total_states = transitions.shape
    m = states * actions
    flat_rows = transitions.reshape(m, total_states)
    near = functools.partial(pltpu.with_memory_space_constraint, memory_space=pltpu.HBM)
    value, spread, ref_rows = call(
        begin_kernel,
        "begin",
        [SMEM, HBM, VMEM],
        [TILE, SPREAD, jax.ShapeDtypeStruct((ROWS, LANES), jnp.int32)],
        [pltpu.VMEM(start_values.shape, jnp.float32), pltpu.SemaphoreType.DMA],
    )(ref_state, near(start_values), swap(start_values))
    flat_rows, value, spread, their_counts, their_costs = lax.optimization_barrier(
        (flat_rows, value, spread, swap(valid_counts), swap(costs))
    )
    their_rows = swap(flat_rows)
    my_rows = near(flat_rows)
    parts = pltpu.VMEM((2, m, total_states), jnp.bfloat16)
    field = pltpu.VMEM((total_states, LANES), jnp.bfloat16)
    count = 4
    old = gather(spread)
    spread, mine, theirs, costs = call(
        first_kernel,
        "bellman_0",
        [VMEM, HBM, VMEM, HBM, SMEM, HBM, VMEM],
        [SPREAD, parts, parts, pltpu.VMEM((m, LANES), jnp.float32)],
        [
            field,
            pltpu.VMEM((count, m, total_states // count), jnp.float32),
            pltpu.SMEM(valid_counts.shape, jnp.int32),
            pltpu.VMEM(costs.shape, jnp.float32),
            pltpu.SemaphoreType.DMA((count,)),
            pltpu.SemaphoreType.DMA((2,)),
        ],
        32,
    )(old, my_rows, their_rows, near(valid_counts), their_counts, near(costs), their_costs)
    mine = pltpu.with_memory_space_constraint(mine, pltpu.VMEM)
    theirs = pltpu.with_memory_space_constraint(theirs, pltpu.VMEM)
    ends_shape = jax.ShapeDtypeStruct((2 * ITERS, LANES), jnp.float32)
    ends = value
    for t in range(1, ITERS):
        last = t == ITERS - 1
        blocks = gather(spread)
        pairs = jax.ShapeDtypeStruct((YS * ZS * XS, 2, LANES), jnp.float32)
        outs = call(
            functools.partial(bellman_kernel, t),
            f"bellman_{t}",
            [VMEM] * (8 if last else 6),
            [TILE, pairs, ends_shape] if last else [SPREAD, ends_shape],
            [field],
        )(blocks, old, mine, theirs, costs, ends, *([ref_rows, spread] if last else []))
        spread, ends = outs[-2:]
        old = blocks
    rows = lax.all_to_all(spread, ("y", "z", "x"), 0, 0, tiled=True)
    packet = call(packet_kernel, "packet", [VMEM] * 3, jax.ShapeDtypeStruct((ROWS + 2 * ITERS, LANES), jnp.float32))(
        rows, outs[0], ends
    )
    bound = jax.ShapeDtypeStruct((ITERS, LANES), jnp.float32)
    return tuple(call(unpack_kernel, "unpack", [VMEM] * 2, [TILE, bound, bound])(packet, swap(packet)))


def solution(mesh):
    split = Mesh(mesh.devices.reshape(YS, ZS, XS, CS), AXES)
    return jax.shard_map(
        local,
        mesh=split,
        in_specs=(P(AXES, None, None), P(AXES, None, None), P(AXES), P(AXES, None), P()),
        out_specs=(P(AXES, None), P(), P()),
        check_vma=False,
    )
```

```python
import functools

import jax
import jax.numpy as jnp
from jax import lax
from jax.experimental import pallas as pl
from jax.experimental.pallas import tpu as pltpu
from jax.sharding import Mesh
from jax.sharding import PartitionSpec as P

ITERS = 4
YS, ZS, XS, CS = 4, 8, 4, 2
ROWS = 16
HALF = 64
LANES = 128
AXES = ("y", "z", "x", "c")
SWAP = [(0, 1), (1, 0)]
big_value = 1e30

VMEM = pl.BlockSpec(memory_space=pltpu.VMEM)
SMEM = pl.BlockSpec(memory_space=pltpu.SMEM)
HBM = pl.BlockSpec(memory_space=pltpu.HBM)
TILE = jax.ShapeDtypeStruct((ROWS, LANES), jnp.float32)
SPREAD = jax.ShapeDtypeStruct((ZS, ROWS, LANES), jnp.float32)


def half_of(shape):
    return lax.broadcasted_iota(jnp.int32, shape, len(shape) - 1) // HALF


def merge(core, mine, theirs):
    return jnp.where(half_of(mine.shape) == core, mine, pltpu.roll(theirs, HALF, mine.ndim - 1))


def call(body, name, ins, outs, scratch=(), mib=16):
    return pl.pallas_call(
        body,
        in_specs=ins,
        out_specs=[VMEM] * len(outs) if isinstance(outs, list) else VMEM,
        out_shape=outs,
        scratch_shapes=scratch,
        compiler_params=pltpu.CompilerParams(vmem_limit_bytes=mib << 20),
        name=name,
    )


def begin_kernel(ref_ref, my_start_hbm, their_start_ref, value_ref, spread_ref, ref_out, my_start_ref, sem):
    copy = pltpu.make_async_copy(my_start_hbm, my_start_ref, sem)
    copy.start()
    ref_out[...] = jnp.full((ROWS, LANES), ref_ref[0], jnp.int32)
    copy.wait()
    value = merge(lax.axis_index("c"), my_start_ref[...], their_start_ref[...])
    value_ref[...] = value
    for i in range(ZS):
        spread_ref[i] = value


def base_of(blocks_ref):
    row = blocks_ref[0, 0:1, :]
    return jnp.where(half_of((1, LANES)) == 0, row, pltpu.roll(row, HALF, 1))


def place(blocks_ref, field, old_ref=None):
    left = half_of((ROWS, LANES)) == 0
    base = jnp.broadcast_to(base_of(blocks_ref), (ROWS, LANES))
    high_end = low_end = None
    for i in range(YS * ZS * XS):
        y, z, x = i // (ZS * XS), i // XS % ZS, i % XS
        block = (y * XS + x, slice(z * ROWS, (z + 1) * ROWS))
        v = blocks_ref[block]
        if old_ref is not None:
            increase = v - old_ref[block]
            high_end = increase if i == 0 else jnp.maximum(high_end, increase)
            low_end = increase if i == 0 else jnp.minimum(low_end, increase)
        v = v - base
        high = v.astype(jnp.bfloat16).astype(jnp.float32)
        low = v - high
        at = i * CS * ROWS
        field[at : at + ROWS, :] = jnp.where(left, high, pltpu.roll(low, HALF, 1)).astype(jnp.bfloat16)
        field[at + ROWS : at + 2 * ROWS, :] = jnp.where(left, pltpu.roll(high, HALF, 1), low).astype(jnp.bfloat16)
    if old_ref is None:
        return None
    old_base = base_of(old_ref)
    up = both_halves(jnp.max(high_end, axis=0, keepdims=True)) + old_base
    down = both_halves(jnp.max(-low_end, axis=0, keepdims=True)) - old_base
    return up, down


def both_halves(row):
    return jnp.maximum(row, pltpu.roll(row, HALF, 1))


def product(high, low, field):
    total = jnp.dot(high, field, preferred_element_type=jnp.float32)
    return total + jnp.dot(low, field, preferred_element_type=jnp.float32)


def improve(mine, theirs, costs):
    mine = mine + pltpu.roll(mine, HALF, 1)
    theirs = theirs + pltpu.roll(theirs, HALF, 1)
    q = costs + jnp.where(half_of(mine.shape) == lax.axis_index("c"), mine, theirs)
    return jnp.min(q.reshape(ROWS, q.shape[0] // ROWS, LANES), axis=1)


def first_kernel(
    blocks_ref, mine_hbm, theirs_ref, my_counts_hbm, their_counts_ref, my_costs_hbm, their_costs_ref,
    spread_ref, mine_out, theirs_out, costs_out,
    field, mine_rows, my_counts_ref, my_costs_ref, sems, small_sems,
):
    small = [
        pltpu.make_async_copy(my_counts_hbm, my_counts_ref, small_sems.at[0]),
        pltpu.make_async_copy(my_costs_hbm, my_costs_ref, small_sems.at[1]),
    ]
    for copy in small:
        copy.start()
    wide = mine_rows.shape[2]
    copies = []
    for j in range(mine_rows.shape[0]):
        copy = pltpu.make_async_copy(mine_hbm.at[:, pl.ds(j * wide, wide)], mine_rows.at[j], sems.at[j])
        copy.start()
        copies.append(copy)
    place(blocks_ref, field)

    def part(p, out, j):
        at = slice(j * wide, (j + 1) * wide)
        high = p.astype(jnp.bfloat16)
        low = (p - high.astype(jnp.float32)).astype(jnp.bfloat16)
        out[0, :, at] = high
        out[1, :, at] = low
        return product(high, low, field[at, :])

    for copy in small:
        copy.wait()
    core = lax.axis_index("c")
    actions = my_costs_ref.shape[1]
    action = lax.broadcasted_iota(jnp.int32, (actions, LANES), 0)
    for s in range(ROWS):
        own = jnp.where(action < my_counts_ref[s], my_costs_ref[s], big_value)
        other = jnp.where(action < their_counts_ref[s], their_costs_ref[s], big_value)
        costs_out[s * actions : (s + 1) * actions, :] = merge(core, own, other)
    theirs = mine = 0.0
    for j in range(len(copies)):
        theirs = theirs + part(theirs_ref[:, j * wide : (j + 1) * wide], theirs_out, j)
    for j, copy in enumerate(copies):
        copy.wait()
        mine = mine + part(mine_rows[j], mine_out, j)
    best = improve(mine, theirs, costs_out[...])
    for i in range(ZS):
        spread_ref[i] = best


def bellman_kernel(t, blocks_ref, old_ref, mine_ref, theirs_ref, costs_ref, ends_ref, *refs):
    last = t == ITERS - 1
    spread_ref, ends_out, field = refs[-3:]
    up, down = place(blocks_ref, field, old_ref)
    mine = product(mine_ref[0], mine_ref[1], field[...])
    theirs = product(theirs_ref[0], theirs_ref[1], field[...])
    best = improve(mine, theirs, costs_ref[...])
    row = lax.broadcasted_iota(jnp.int32, (2 * ITERS, LANES), 0)
    ends = jnp.zeros((2 * ITERS, LANES), jnp.float32) if t == 1 else ends_ref[...]
    ends = jnp.where(row == t - 1, up, ends)
    ends_out[...] = jnp.where(row == ITERS + t - 1, down, ends)
    if not last:
        for i in range(ZS):
            spread_ref[i] = best
        return
    ref_ref, value_ref, best_ref = refs[:3]
    increase = best - (value_ref[0] - base_of(blocks_ref))
    up = both_halves(jnp.max(increase, axis=0, keepdims=True))
    down = both_halves(jnp.max(-increase, axis=0, keepdims=True))
    chip = (lax.axis_index("y") * ZS + lax.axis_index("z")) * XS + lax.axis_index("x")
    state = lax.broadcasted_iota(jnp.int32, (ROWS, LANES), 0) + ROWS * (CS * chip + half_of((ROWS, LANES)))
    ref_row = both_halves(jnp.max(jnp.where(state == ref_ref[...], best, -big_value), axis=0, keepdims=True))
    best_ref[...] = best
    pair = jnp.concatenate([jnp.where(half_of((1, LANES)) == 0, up, down), ref_row], axis=0)
    spread_ref[...] = jnp.broadcast_to(pair[None], spread_ref.shape)


def packet_kernel(parts_ref, value_ref, ends_ref, out_ref):
    pair = jnp.max(parts_ref[...], axis=0)
    out_ref[0:ROWS, :] = value_ref[...] - pair[1:2, :]
    turned = pltpu.roll(pair, HALF, 1)
    left = half_of((1, LANES)) == 0
    row = lax.broadcasted_iota(jnp.int32, (2 * ITERS, LANES), 0)
    ends = jnp.where(row == ITERS - 1, jnp.where(left, pair[0:1, :], turned[0:1, :]), ends_ref[...])
    ends = jnp.where(row == 2 * ITERS - 1, jnp.where(left, turned[0:1, :], pair[0:1, :]), ends)
    out_ref[ROWS : ROWS + 2 * ITERS, :] = ends


def unpack_kernel(mine_ref, theirs_ref, relative_ref, lower_ref, upper_ref):
    core = lax.axis_index("c")
    relative_ref[...] = merge(core, mine_ref[0:ROWS, :], theirs_ref[0:ROWS, :])
    bounds = jnp.where(
        half_of((2 * ITERS, LANES)) == core,
        mine_ref[ROWS : ROWS + 2 * ITERS, :],
        theirs_ref[ROWS : ROWS + 2 * ITERS, :],
    )
    upper_ref[...] = bounds[:ITERS]
    lower_ref[...] = -bounds[ITERS:]


def gather(spread):
    block = lax.all_to_all(spread, "z", 0, 0, tiled=True).reshape(1, ZS * ROWS, LANES)
    plane = jnp.broadcast_to(block, (YS * XS, ZS * ROWS, LANES))
    return lax.all_to_all(plane, ("y", "x"), 0, 0, tiled=True)


def swap(value):
    return lax.ppermute(value, "c", SWAP)


def local(transitions, costs, valid_counts, start_values, ref_state):
    states, actions, total_states = transitions.shape
    m = states * actions
    flat_rows = transitions.reshape(m, total_states)
    near = functools.partial(pltpu.with_memory_space_constraint, memory_space=pltpu.HBM)
    value, spread, ref_rows = call(
        begin_kernel,
        "begin",
        [SMEM, HBM, VMEM],
        [TILE, SPREAD, jax.ShapeDtypeStruct((ROWS, LANES), jnp.int32)],
        [pltpu.VMEM(start_values.shape, jnp.float32), pltpu.SemaphoreType.DMA],
    )(ref_state, near(start_values), swap(start_values))
    flat_rows, value, spread, their_counts, their_costs = lax.optimization_barrier(
        (flat_rows, value, spread, swap(valid_counts), swap(costs))
    )
    their_rows = swap(flat_rows)
    my_rows = near(flat_rows)
    parts = pltpu.VMEM((2, m, total_states), jnp.bfloat16)
    field = pltpu.VMEM((total_states, LANES), jnp.bfloat16)
    count = 4
    old = gather(spread)
    spread, mine, theirs, costs = call(
        first_kernel,
        "bellman_0",
        [VMEM, HBM, VMEM, HBM, SMEM, HBM, VMEM],
        [SPREAD, parts, parts, pltpu.VMEM((m, LANES), jnp.float32)],
        [
            field,
            pltpu.VMEM((count, m, total_states // count), jnp.float32),
            pltpu.SMEM(valid_counts.shape, jnp.int32),
            pltpu.VMEM(costs.shape, jnp.float32),
            pltpu.SemaphoreType.DMA((count,)),
            pltpu.SemaphoreType.DMA((2,)),
        ],
        32,
    )(old, my_rows, their_rows, near(valid_counts), their_counts, near(costs), their_costs)
    mine = pltpu.with_memory_space_constraint(mine, pltpu.VMEM)
    theirs = pltpu.with_memory_space_constraint(theirs, pltpu.VMEM)
    ends_shape = jax.ShapeDtypeStruct((2 * ITERS, LANES), jnp.float32)
    ends = value
    for t in range(1, ITERS):
        last = t == ITERS - 1
        blocks = gather(spread)
        pairs = jax.ShapeDtypeStruct((YS * ZS * XS, 2, LANES), jnp.float32)
        outs = call(
            functools.partial(bellman_kernel, t),
            f"bellman_{t}",
            [VMEM] * (8 if last else 6),
            [TILE, pairs, ends_shape] if last else [SPREAD, ends_shape],
            [field],
        )(blocks, old, mine, theirs, costs, ends, *([ref_rows, spread] if last else []))
        spread, ends = outs[-2:]
        old = blocks
    rows = lax.all_to_all(spread, ("y", "z", "x"), 0, 0, tiled=True)
    packet = call(packet_kernel, "packet", [VMEM] * 3, jax.ShapeDtypeStruct((ROWS + 2 * ITERS, LANES), jnp.float32))(
        rows, outs[0], ends
    )
    bound = jax.ShapeDtypeStruct((ITERS, LANES), jnp.float32)
    return tuple(call(unpack_kernel, "unpack", [VMEM] * 2, [TILE, bound, bound])(packet, swap(packet)))


def solution(mesh):
    split = Mesh(mesh.devices.reshape(YS, ZS, XS, CS), AXES)
    return jax.shard_map(
        local,
        mesh=split,
        in_specs=(P(AXES, None, None), P(AXES, None, None), P(AXES), P(AXES, None), P()),
        out_specs=(P(AXES, None), P(), P()),
        check_vma=False,
    )
```

```python
import functools

import jax
import jax.numpy as jnp
from jax import lax
from jax.experimental import pallas as pl
from jax.experimental.pallas import tpu as pltpu
from jax.sharding import Mesh
from jax.sharding import PartitionSpec as P

ITERS = 4
YS, ZS, XS, CS = 4, 8, 4, 2
ROWS = 16
HALF = 64
LANES = 128
AXES = ("y", "z", "x", "c")
SWAP = [(0, 1), (1, 0)]
big_value = 1e30

VMEM = pl.BlockSpec(memory_space=pltpu.VMEM)
SMEM = pl.BlockSpec(memory_space=pltpu.SMEM)
HBM = pl.BlockSpec(memory_space=pltpu.HBM)
TILE = jax.ShapeDtypeStruct((ROWS, LANES), jnp.float32)
SPREAD = jax.ShapeDtypeStruct((ZS, ROWS, LANES), jnp.float32)


def half_of(shape):
    return lax.broadcasted_iota(jnp.int32, shape, len(shape) - 1) // HALF


def merge(core, mine, theirs):
    return jnp.where(half_of(mine.shape) == core, mine, pltpu.roll(theirs, HALF, mine.ndim - 1))


def call(body, name, ins, outs, scratch=(), mib=16):
    return pl.pallas_call(
        body,
        in_specs=ins,
        out_specs=[VMEM] * len(outs) if isinstance(outs, list) else VMEM,
        out_shape=outs,
        scratch_shapes=scratch,
        compiler_params=pltpu.CompilerParams(vmem_limit_bytes=mib << 20),
        name=name,
    )


def begin_kernel(ref_ref, my_start_hbm, their_start_ref, value_ref, spread_ref, ref_out, my_start_ref, sem):
    copy = pltpu.make_async_copy(my_start_hbm, my_start_ref, sem)
    copy.start()
    ref_out[...] = jnp.full((ROWS, LANES), ref_ref[0], jnp.int32)
    copy.wait()
    value = merge(lax.axis_index("c"), my_start_ref[...], their_start_ref[...])
    value_ref[...] = value
    for i in range(ZS):
        spread_ref[i] = value


def base_of(blocks_ref):
    row = blocks_ref[0, 0:1, :]
    return jnp.where(half_of((1, LANES)) == 0, row, pltpu.roll(row, HALF, 1))


def place(blocks_ref, field, old_ref=None):
    left = half_of((ROWS, LANES)) == 0
    base = jnp.broadcast_to(base_of(blocks_ref), (ROWS, LANES))
    high_end = low_end = None
    for i in range(YS * ZS * XS):
        y, z, x = i // (ZS * XS), i // XS % ZS, i % XS
        block = (y * XS + x, slice(z * ROWS, (z + 1) * ROWS))
        v = blocks_ref[block]
        if old_ref is not None:
            increase = v - old_ref[block]
            high_end = increase if i == 0 else jnp.maximum(high_end, increase)
            low_end = increase if i == 0 else jnp.minimum(low_end, increase)
        v = v - base
        high = v.astype(jnp.bfloat16).astype(jnp.float32)
        low = v - high
        at = i * CS * ROWS
        field[at : at + ROWS, :] = jnp.where(left, high, pltpu.roll(low, HALF, 1)).astype(jnp.bfloat16)
        field[at + ROWS : at + 2 * ROWS, :] = jnp.where(left, pltpu.roll(high, HALF, 1), low).astype(jnp.bfloat16)
    if old_ref is None:
        return None
    old_base = base_of(old_ref)
    up = both_halves(jnp.max(high_end, axis=0, keepdims=True)) + old_base
    down = both_halves(jnp.max(-low_end, axis=0, keepdims=True)) - old_base
    return up, down


def both_halves(row):
    return jnp.maximum(row, pltpu.roll(row, HALF, 1))


def product(high, low, field):
    total = jnp.dot(high, field, preferred_element_type=jnp.float32)
    return total + jnp.dot(low, field, preferred_element_type=jnp.float32)


def improve(mine, theirs, costs):
    mine = mine + pltpu.roll(mine, HALF, 1)
    theirs = theirs + pltpu.roll(theirs, HALF, 1)
    q = costs + jnp.where(half_of(mine.shape) == lax.axis_index("c"), mine, theirs)
    return jnp.min(q.reshape(ROWS, q.shape[0] // ROWS, LANES), axis=1)


def first_kernel(
    blocks_ref, mine_hbm, theirs_ref, my_counts_hbm, their_counts_ref, my_costs_hbm, their_costs_ref,
    spread_ref, mine_out, theirs_out, costs_out,
    field, mine_rows, my_counts_ref, my_costs_ref, sems, small_sems,
):
    small = [
        pltpu.make_async_copy(my_counts_hbm, my_counts_ref, small_sems.at[0]),
        pltpu.make_async_copy(my_costs_hbm, my_costs_ref, small_sems.at[1]),
    ]
    for copy in small:
        copy.start()
    wide = mine_rows.shape[2]
    copies = []
    for j in range(mine_rows.shape[0]):
        copy = pltpu.make_async_copy(mine_hbm.at[:, pl.ds(j * wide, wide)], mine_rows.at[j], sems.at[j])
        copy.start()
        copies.append(copy)
    place(blocks_ref, field)

    def part(p, out, j):
        at = slice(j * wide, (j + 1) * wide)
        high = p.astype(jnp.bfloat16)
        low = (p - high.astype(jnp.float32)).astype(jnp.bfloat16)
        out[0, :, at] = high
        out[1, :, at] = low
        return product(high, low, field[at, :])

    for copy in small:
        copy.wait()
    core = lax.axis_index("c")
    actions = my_costs_ref.shape[1]
    action = lax.broadcasted_iota(jnp.int32, (actions, LANES), 0)
    for s in range(ROWS):
        own = jnp.where(action < my_counts_ref[s], my_costs_ref[s], big_value)
        other = jnp.where(action < their_counts_ref[s], their_costs_ref[s], big_value)
        costs_out[s * actions : (s + 1) * actions, :] = merge(core, own, other)
    theirs = mine = 0.0
    for j in range(len(copies)):
        theirs = theirs + part(theirs_ref[:, j * wide : (j + 1) * wide], theirs_out, j)
    for j, copy in enumerate(copies):
        copy.wait()
        mine = mine + part(mine_rows[j], mine_out, j)
    best = improve(mine, theirs, costs_out[...])
    for i in range(ZS):
        spread_ref[i] = best


def bellman_kernel(t, blocks_ref, old_ref, mine_ref, theirs_ref, costs_ref, ends_ref, *refs):
    last = t == ITERS - 1
    spread_ref, ends_out, field = refs[-3:]
    up, down = place(blocks_ref, field, old_ref)
    mine = product(mine_ref[0], mine_ref[1], field[...])
    theirs = product(theirs_ref[0], theirs_ref[1], field[...])
    best = improve(mine, theirs, costs_ref[...])
    row = lax.broadcasted_iota(jnp.int32, (2 * ITERS, LANES), 0)
    ends = jnp.zeros((2 * ITERS, LANES), jnp.float32) if t == 1 else ends_ref[...]
    ends = jnp.where(row == t - 1, up, ends)
    ends_out[...] = jnp.where(row == ITERS + t - 1, down, ends)
    if not last:
        for i in range(ZS):
            spread_ref[i] = best
        return
    ref_ref, value_ref, best_ref = refs[:3]
    increase = best - (value_ref[0] - base_of(blocks_ref))
    up = both_halves(jnp.max(increase, axis=0, keepdims=True))
    down = both_halves(jnp.max(-increase, axis=0, keepdims=True))
    chip = (lax.axis_index("y") * ZS + lax.axis_index("z")) * XS + lax.axis_index("x")
    state = lax.broadcasted_iota(jnp.int32, (ROWS, LANES), 0) + ROWS * (CS * chip + half_of((ROWS, LANES)))
    ref_row = both_halves(jnp.max(jnp.where(state == ref_ref[...], best, -big_value), axis=0, keepdims=True))
    best_ref[...] = best
    pair = jnp.concatenate([jnp.where(half_of((1, LANES)) == 0, up, down), ref_row], axis=0)
    spread_ref[...] = jnp.broadcast_to(pair[None], spread_ref.shape)


def packet_kernel(parts_ref, value_ref, ends_ref, out_ref):
    pair = jnp.max(parts_ref[...], axis=0)
    out_ref[0:ROWS, :] = value_ref[...] - pair[1:2, :]
    turned = pltpu.roll(pair, HALF, 1)
    left = half_of((1, LANES)) == 0
    row = lax.broadcasted_iota(jnp.int32, (2 * ITERS, LANES), 0)
    ends = jnp.where(row == ITERS - 1, jnp.where(left, pair[0:1, :], turned[0:1, :]), ends_ref[...])
    ends = jnp.where(row == 2 * ITERS - 1, jnp.where(left, turned[0:1, :], pair[0:1, :]), ends)
    out_ref[ROWS : ROWS + 2 * ITERS, :] = ends


def unpack_kernel(mine_ref, theirs_ref, relative_ref, lower_ref, upper_ref):
    core = lax.axis_index("c")
    relative_ref[...] = merge(core, mine_ref[0:ROWS, :], theirs_ref[0:ROWS, :])
    bounds = jnp.where(
        half_of((2 * ITERS, LANES)) == core,
        mine_ref[ROWS : ROWS + 2 * ITERS, :],
        theirs_ref[ROWS : ROWS + 2 * ITERS, :],
    )
    upper_ref[...] = bounds[:ITERS]
    lower_ref[...] = -bounds[ITERS:]


def gather(spread):
    block = lax.all_to_all(spread, "z", 0, 0, tiled=True).reshape(1, ZS * ROWS, LANES)
    plane = jnp.broadcast_to(block, (YS * XS, ZS * ROWS, LANES))
    return lax.all_to_all(plane, ("y", "x"), 0, 0, tiled=True)


def swap(value):
    return lax.ppermute(value, "c", SWAP)


def local(transitions, costs, valid_counts, start_values, ref_state):
    states, actions, total_states = transitions.shape
    m = states * actions
    flat_rows = transitions.reshape(m, total_states)
    near = functools.partial(pltpu.with_memory_space_constraint, memory_space=pltpu.HBM)
    value, spread, ref_rows = call(
        begin_kernel,
        "begin",
        [SMEM, HBM, VMEM],
        [TILE, SPREAD, jax.ShapeDtypeStruct((ROWS, LANES), jnp.int32)],
        [pltpu.VMEM(start_values.shape, jnp.float32), pltpu.SemaphoreType.DMA],
    )(ref_state, near(start_values), swap(start_values))
    flat_rows, value, spread, their_counts, their_costs = lax.optimization_barrier(
        (flat_rows, value, spread, swap(valid_counts), swap(costs))
    )
    their_rows = swap(flat_rows)
    my_rows = near(flat_rows)
    parts = pltpu.VMEM((2, m, total_states), jnp.bfloat16)
    field = pltpu.VMEM((total_states, LANES), jnp.bfloat16)
    count = 2
    old = gather(spread)
    spread, mine, theirs, costs = call(
        first_kernel,
        "bellman_0",
        [VMEM, HBM, VMEM, HBM, SMEM, HBM, VMEM],
        [SPREAD, parts, parts, pltpu.VMEM((m, LANES), jnp.float32)],
        [
            field,
            pltpu.VMEM((count, m, total_states // count), jnp.float32),
            pltpu.SMEM(valid_counts.shape, jnp.int32),
            pltpu.VMEM(costs.shape, jnp.float32),
            pltpu.SemaphoreType.DMA((count,)),
            pltpu.SemaphoreType.DMA((2,)),
        ],
        32,
    )(old, my_rows, their_rows, near(valid_counts), their_counts, near(costs), their_costs)
    mine = pltpu.with_memory_space_constraint(mine, pltpu.VMEM)
    theirs = pltpu.with_memory_space_constraint(theirs, pltpu.VMEM)
    ends_shape = jax.ShapeDtypeStruct((2 * ITERS, LANES), jnp.float32)
    ends = value
    for t in range(1, ITERS):
        last = t == ITERS - 1
        blocks = gather(spread)
        pairs = jax.ShapeDtypeStruct((YS * ZS * XS, 2, LANES), jnp.float32)
        outs = call(
            functools.partial(bellman_kernel, t),
            f"bellman_{t}",
            [VMEM] * (8 if last else 6),
            [TILE, pairs, ends_shape] if last else [SPREAD, ends_shape],
            [field],
        )(blocks, old, mine, theirs, costs, ends, *([ref_rows, spread] if last else []))
        spread, ends = outs[-2:]
        old = blocks
    rows = lax.all_to_all(spread, ("y", "z", "x"), 0, 0, tiled=True)
    packet = call(packet_kernel, "packet", [VMEM] * 3, jax.ShapeDtypeStruct((ROWS + 2 * ITERS, LANES), jnp.float32))(
        rows, outs[0], ends
    )
    bound = jax.ShapeDtypeStruct((ITERS, LANES), jnp.float32)
    return tuple(call(unpack_kernel, "unpack", [VMEM] * 2, [TILE, bound, bound])(packet, swap(packet)))


def solution(mesh):
    split = Mesh(mesh.devices.reshape(YS, ZS, XS, CS), AXES)
    return jax.shard_map(
        local,
        mesh=split,
        in_specs=(P(AXES, None, None), P(AXES, None, None), P(AXES), P(AXES, None), P()),
        out_specs=(P(AXES, None), P(), P()),
        check_vma=False,
    )
```
